32 devices in a mesh: groups: 2 (over x), space: 4 (over y, core), frame: 4 (over z).
Axes of the slice: x: 2, y: 2, z: 4, core: 2. Of those that a mesh axis runs over, the one named last changes fastest.
Arguments:
- tokens: bfloat16 [4, 64, 128, 512], P('frame', ('groups', 'space')), parts along dimension 1, may hold values from -6 to 6
- src_brick: int32 [3, 64], P(None, 'groups'), parts along dimension 1, may hold values from 0 to 31, as said below
- merge_num: int32 [3, 64], P(None, 'groups'), parts along dimension 1, may hold values from 1 to 4
- gain_attn: float32 [512], replicated, may hold values from 0.1 to 1.9
- w_query: bfloat16 [512, 512], replicated, may hold values from -4 to 4
- w_key: bfloat16 [512, 512], replicated, may hold values from -4 to 4
- w_value: bfloat16 [512, 512], replicated, may hold values from -0.25 to 0.25
- w_out: bfloat16 [512, 512], replicated, may hold values from -0.25 to 0.25
- gain_mlp: float32 [512], replicated, may hold values from 0.1 to 1.9
- w_in: bfloat16 [512, 2048], replicated, may hold values from -0.25 to 0.25
- w_back: bfloat16 [2048, 512], replicated, may hold values from -0.125 to 0.125
Outputs:
- output: bfloat16 [4, 64, 128, 512], P('frame', ('groups', 'space')), parts along dimension 1
The draws below stay inside these ranges and needn't reach their ends.
There are 2 independent parts, one for each index of `groups`. The reference program is written for one: setup_inputs(seed, part) draws one part's arguments, and reference() takes and returns one part's arrays. A program takes and returns all parts, laid end to end along the dimension named above; an argument that names none is the same for every part. Nothing has to cross between parts.
Inputs may be any that keep to these rules, and one draw needn't show every extreme that they name: `src_brick`: group the bricks in aligned groups of 8. Over all frames, at most 7 entries pair a target brick of one group with a source brick of one group, and for every target group some source group is paired exactly 7 times.
All inputs are finite; a program needn't handle non-finite values.
Results may differ from the reference program's by a relative error of at most 0.0069.
Values may be sent and summed in bfloat16 or wider, within the bound.
A program may use at most 64 MiB of HBM per device.

```python
import jax
import jax.numpy as jnp
from jax import lax

D = 512
HD = 64
FF = 2048
BT = 128
BR_DEV = 8
FRAMES = 4
BRICKS = 32
CAP = 7


def draw_src_brick(key, part):
    groups_all = BRICKS // BR_DEV
    request_total = (FRAMES - 1) * BR_DEV
    slot_total = groups_all * CAP

    def draw_row(requester):
        row_key = jax.random.fold_in(key, requester)
        key_hot, key_mix, key_order, key_pick = jax.random.split(row_key, 4)
        hot_owner = (requester + jax.random.randint(key_hot, (), -1, 2)) % groups_all
        owner_of = jnp.arange(slot_total) // CAP
        shuffle = jax.random.permutation(key_mix, slot_total)
        scores = jnp.where(owner_of == hot_owner, jnp.arange(slot_total), slot_total + shuffle)
        ordering = jnp.argsort(scores)
        chosen = owner_of[ordering[:request_total]]
        chosen = chosen[jax.random.permutation(key_order, request_total)]
        local_pick = jax.random.randint(key_pick, (request_total,), 0, BR_DEV)
        return (chosen * BR_DEV + local_pick).reshape(FRAMES - 1, BR_DEV)
    src_table = jax.vmap(draw_row)(jnp.arange(groups_all))
    return jnp.transpose(src_table, (1, 0, 2)).reshape(FRAMES - 1, BRICKS).astype(jnp.int32)


def projection(key, salt):
    noise_draw = jax.random.normal(jax.random.fold_in(key, salt), (D, D), jnp.float32)
    matrix_out = noise_draw * D ** (-0.5)
    return matrix_out.astype(jnp.bfloat16)


def draw_w_query(key, part):
    return projection(key, 21)


def draw_w_key(key, part):
    return projection(key, 22)


def place_ends(values, rng, least, high):
    dims = values.shape
    spot = [jax.random.randint(jax.random.fold_in(rng, axis), (), 0, dims[axis]) for axis in range(len(dims))]
    values = values.at[tuple(spot)].set(least)
    longest = dims.index(max(dims))
    spot[longest] = (spot[longest] + 1) % dims[longest]
    return values.at[tuple(spot)].set(high)


def block_levels(own_key, dims, shards, smallest, top_value):
    factor_of = 1.0
    for dim, parts in shards:
        steps = jax.random.uniform(jax.random.fold_in(jax.random.fold_in(own_key, 6), dim), (parts,), jnp.float32, smallest / len(shards), top_value / len(shards))
        factor_of = factor_of * jnp.repeat(jnp.exp(steps), dims[dim] // parts).reshape((-1,) + (1,) * (len(dims) - 1 - dim))
    return factor_of


def centred(own_key, shape, deviation, bound, shards=(), kind=jnp.bfloat16):
    drawn = jax.random.normal(own_key, shape, jnp.float32) * deviation
    if len(shards) > 0:
        drawn = block_levels(own_key, shape, shards, -0.22, 0.18) * drawn
    return jnp.clip(drawn, min=-bound, max=bound).astype(kind)


def setup_inputs(seed: int = 0, part: int = 0) -> dict:
    keys = jax.random.split(jax.random.key(seed), 12)
    part_splits = jax.random.split(jax.random.fold_in(keys[11], part), 12)
    return {
        "tokens": centred(part_splits[0], (FRAMES, BRICKS, BT, D), 1.0, 6.0, ((0, 4), (1, 4))),
        "src_brick": draw_src_brick(jax.random.fold_in(jax.random.fold_in(keys[11], part), 71), part),
        "merge_num": place_ends(jax.random.randint(part_splits[2], (FRAMES - 1, BRICKS), 1, 5), jax.random.fold_in(part_splits[2], 1), 1, 4).astype(jnp.int32),
        "gain_attn": jnp.clip(1.0 + 0.18 * jax.random.normal(keys[3], (D,), jnp.float32), 0.1, 1.9),
        "w_query": draw_w_query(jax.random.fold_in(keys[11], 71), part),
        "w_key": draw_w_key(jax.random.fold_in(keys[11], 71), part),
        "w_value": centred(keys[6], (D, D), D ** -0.5, 0.25),
        "w_out": centred(keys[7], (D, D), D ** -0.5, 0.25),
        "gain_mlp": jnp.clip(1.0 + 0.18 * jax.random.normal(keys[8], (D,), jnp.float32), 0.1, 1.9),
        "w_in": centred(keys[9], (D, FF), D ** -0.5, 0.25),
        "w_back": centred(keys[10], (FF, D), FF ** -0.5, 0.125),
    }


def rms_norm(values_in, gain):
    as_float = values_in.astype(jnp.float32)
    mean_sq = lax.optimization_barrier(jnp.mean(as_float * as_float, axis=-1, keepdims=True))
    return (as_float * lax.rsqrt(mean_sq + 1e-06) * gain.astype(jnp.float32)).astype(jnp.bfloat16)

def temporal_block(merged, gain_attn, w_query, w_key, w_value, w_out, gain_mlp, w_in, w_back):
    frames_all, rows_all = (merged.shape[0], merged.shape[1])
    heads = D // HD
    normed = rms_norm(merged, gain_attn)
    queries = jnp.dot(normed, w_query, preferred_element_type=jnp.float32).astype(jnp.bfloat16)
    keys_proj = jnp.dot(normed, w_key, preferred_element_type=jnp.float32).astype(jnp.bfloat16)
    values_proj = jnp.dot(normed, w_value, preferred_element_type=jnp.float32).astype(jnp.bfloat16)
    query_heads = queries.reshape(frames_all, rows_all, heads, HD).astype(jnp.float32)
    key_heads = keys_proj.reshape(frames_all, rows_all, heads, HD).astype(jnp.float32)
    value_heads = values_proj.reshape(frames_all, rows_all, heads, HD).astype(jnp.float32)
    scores = jnp.einsum('fmhd,gmhd->fghm', query_heads, key_heads) * (1.0 / HD ** 0.5)
    later = jnp.arange(frames_all)[:, None] >= jnp.arange(frames_all)[None, :]
    scores = jnp.where(later[:, :, None, None], scores, -1e+30)
    row_max = lax.optimization_barrier(jnp.max(scores, axis=1, keepdims=True))
    weights_exp = jnp.exp(scores - row_max)
    probs = (weights_exp / lax.optimization_barrier(jnp.sum(weights_exp, axis=1, keepdims=True))).astype(jnp.bfloat16)
    context = jnp.einsum('fghm,gmhd->fmhd', probs.astype(jnp.float32), value_heads)
    context = context.astype(jnp.bfloat16).reshape(frames_all, rows_all, D)
    mid = (merged.astype(jnp.float32) + jnp.dot(context, w_out, preferred_element_type=jnp.float32)).astype(jnp.bfloat16)
    normed2 = rms_norm(mid, gain_mlp)
    hidden = jax.nn.gelu(jnp.dot(normed2, w_in, preferred_element_type=jnp.float32)).astype(jnp.bfloat16)
    return (mid.astype(jnp.float32) + jnp.dot(hidden, w_back, preferred_element_type=jnp.float32)).astype(jnp.bfloat16)

def reference(tokens, src_brick, merge_num, gain_attn, w_query, w_key, w_value, w_out, gain_mlp, w_in, w_back):
    previous = tokens[:-1]
    moved = jax.vmap(lambda frame_rows, picks: jnp.take(frame_rows, picks, axis=0))(previous, src_brick)
    weight = merge_num.astype(jnp.float32) * 0.25
    merged_rest = (tokens[1:].astype(jnp.float32) + weight[:, :, None, None] * moved.astype(jnp.float32)).astype(jnp.bfloat16)
    merged = jnp.concatenate([tokens[:1], merged_rest], axis=0)
    by_brick = jnp.transpose(merged, (1, 0, 2, 3))

    def one_brick(brick_rows):
        return temporal_block(brick_rows, gain_attn, w_query, w_key, w_value, w_out, gain_mlp, w_in, w_back)
    result = lax.map(one_brick, by_brick)
    return jnp.transpose(result, (1, 0, 2, 3))
```

```python
import functools

import jax
import jax.numpy as jnp
from jax import lax
from jax.experimental import pallas as pl
from jax.experimental.pallas import tpu as pltpu
from jax.sharding import PartitionSpec as P

HD = 64
CHUNK = 16
MESH = pl.DeviceIdType.MESH
BF = jnp.bfloat16
F32 = jnp.float32


def norm_rows(values, gain):
    as_float = values.astype(F32)
    mean_sq = jnp.mean(as_float * as_float, axis=-1, keepdims=True)
    return (as_float * lax.rsqrt(mean_sq + 1e-06) * gain).astype(BF)


def matmul(left, right):
    return jnp.dot(left, right, preferred_element_type=F32)


def kernel(dims, *refs):
    n_f, n_s, nb, cr, nc, cap, d = dims
    rows_ref, pick_ref, weight_ref, tok, gain1, gain2 = refs[:6]
    weights_hbm = refs[6:12]
    out = refs[12]
    scratch = list(refs[13:])
    take = lambda count: [scratch.pop(0) for _ in range(count)]
    recv, pack, got, outb = take(nc), take(nc), take(nc), take(nc)
    wq, wk, wv, wo, wi, wb = weights_vmem = take(6)
    merged, nrm, q_s, k_s, v_s, acc = take(6)
    in_send, in_recv, y_send, y_recv, o_send, o_recv, own_in, own_out, wsem = take(9)
    rows = nb * cr
    ff = wi.shape[1]
    zi = lax.axis_index("frame")
    si = lax.axis_index("space")
    span = cr * nc
    f_order = sorted(range(1, n_f), key=lambda k: abs(k - n_f / 2))
    f_peers = [lax.rem(zi + k, n_f) for k in f_order]
    s_peers = [lax.rem(si + k, n_s) for k in range(1, n_s)]

    barrier = pltpu.get_barrier_semaphore()
    for z in f_peers:
        pl.semaphore_signal(barrier, inc=1, device_id={"frame": z}, device_id_type=MESH)
    for s in s_peers:
        pl.semaphore_signal(barrier, inc=1, device_id={"space": s}, device_id_type=MESH)
    pl.semaphore_wait(barrier, n_f - 1 + n_s - 1)

    def tok_at(z, c):
        start = pl.multiple_of(z * span + c * cr, cr)
        return tok.at[0, :, pl.ds(start, cr), :]

    def out_at(z, c):
        start = pl.multiple_of(z * span + c * cr, cr)
        return out.at[0, :, pl.ds(start, cr), :]

    def recv_at(c, f):
        return recv[c].at[pl.ds(f * nb, nb)]

    def in_copy(c, src, dst):
        return pltpu.make_async_remote_copy(
            src_ref=tok_at(dst, c), dst_ref=recv_at(c, src),
            send_sem=in_send.at[c, dst], recv_sem=in_recv.at[c, src],
            device_id={"frame": dst}, device_id_type=MESH)

    def own_in_copy(c):
        return pltpu.make_async_copy(tok_at(zi, c), recv_at(c, zi), own_in.at[c])

    def y_copy(c, src, dst):
        return pltpu.make_async_remote_copy(
            src_ref=pack[c].at[pl.ds(dst * cap, cap)], dst_ref=got[c].at[pl.ds(src * cap, cap)],
            send_sem=y_send.at[c, dst], recv_sem=y_recv.at[c, src],
            device_id={"space": dst}, device_id_type=MESH)

    def o_copy(c, src, dst):
        return pltpu.make_async_remote_copy(
            src_ref=outb[c].at[dst], dst_ref=out_at(src, c),
            send_sem=o_send.at[c, dst], recv_sem=o_recv.at[c, src],
            device_id={"frame": dst}, device_id_type=MESH)

    def own_out_copy(c):
        return pltpu.make_async_copy(outb[c].at[zi], out_at(zi, c), own_out.at[c])

    def weight_copy(i):
        return pltpu.make_async_copy(weights_hbm[i], weights_vmem[i], wsem.at[i])

    for c in range(nc):
        for z in f_peers:
            in_copy(c, zi, z).start()
        own_in_copy(c).start()
    for i in range(6):
        weight_copy(i).start()

    def exchange(c):
        for z in f_peers:
            in_copy(c, z, zi).wait_recv()
        own_in_copy(c).wait()

        def fill(dest, base):
            @pl.loop(0, cap)
            def _(j):
                dest[base + j] = recv[c][rows_ref[base + j]]

        for s in s_peers:
            fill(pack[c], s * cap)
            y_copy(c, si, s).start()
        fill(got[c], si * cap)

    def merge(c):
        for s in s_peers:
            y_copy(c, s, si).wait_recv()

        @pl.loop(0, nb)
        def _(b):
            merged[pl.ds(pl.multiple_of(b * cr, cr), cr), :] = recv[c][b]

        @pl.loop(0, (n_f - 1) * nb)
        def _(r):
            piece = got[c][pick_ref[r]].astype(F32) * weight_ref[r]
            total = recv[c][nb + r].astype(F32) + piece
            merged[pl.ds(pl.multiple_of((nb + r) * cr, cr), cr), :] = total.astype(BF)

    lane_a = lax.broadcasted_iota(jnp.int32, (4 * HD, 4 * HD), 0) // HD
    lane_b = lax.broadcasted_iota(jnp.int32, (4 * HD, 4 * HD), 1) // HD
    head_sum = jnp.where(lane_a == lane_b, 1.0 / HD**0.5, 0.0).astype(BF)

    def attend():
        nrm[...] = norm_rows(merged[...], gain1[...])
        q_s[...] = matmul(nrm[...], wq[...]).astype(BF)
        k_s[...] = matmul(nrm[...], wk[...]).astype(BF)
        v_s[...] = matmul(nrm[...], wv[...]).astype(BF)
        for f in range(n_f):
            here = slice(f * rows, (f + 1) * rows)
            for h in range(d // (4 * HD)):
                lanes = slice(h * 4 * HD, (h + 1) * 4 * HD)
                query = q_s[here, lanes].astype(F32)
                scores = []
                for g in range(f + 1):
                    prod = query * k_s[g * rows : (g + 1) * rows, lanes].astype(F32)
                    high = prod.astype(BF)
                    low = (prod - high.astype(F32)).astype(BF)
                    scores.append(matmul(high, head_sum) + matmul(low, head_sum))
                top = functools.reduce(jnp.maximum, scores)
                exps = [jnp.exp(s - top) for s in scores]
                inverse = 1.0 / functools.reduce(jnp.add, exps)
                total = 0.0
                for g in range(f + 1):
                    prob = (exps[g] * inverse).astype(BF).astype(F32)
                    total = total + prob * v_s[g * rows : (g + 1) * rows, lanes].astype(F32)
                nrm[here, lanes] = total.astype(BF)
        mid = (merged[...].astype(F32) + matmul(nrm[...], wo[...])).astype(BF)
        merged[...] = mid
        nrm[...] = norm_rows(mid, gain2[...])

    def feed(c):
        acc[...] = merged[...].astype(F32)

        @pl.loop(0, ff // d)
        def _(j):
            cols = pl.ds(pl.multiple_of(j * d, d), d)
            hidden = jax.nn.gelu(matmul(nrm[...], wi[:, cols])).astype(BF)
            acc[...] += matmul(hidden, wb[cols, :])

        outb[c][...] = acc[...].astype(BF).reshape(n_f, nb, cr, d)
        for z in f_peers:
            o_copy(c, zi, z).start()
        own_out_copy(c).start()

    exchange(0)
    for i in range(6):
        weight_copy(i).wait()
    for c in range(nc):
        merge(c)
        attend()
        if c + 1 < nc:
            exchange(c + 1)
        feed(c)

    for c in range(nc):
        for z in f_peers:
            in_copy(c, zi, z).wait_send()
            o_copy(c, zi, z).wait_send()
            o_copy(c, z, zi).wait_recv()
        own_out_copy(c).wait()
        for s in s_peers:
            y_copy(c, si, s).wait_send()


def slot_tables(src_brick, n_s, nb, cap, self_index):
    steps = src_brick.shape[0]
    request_total = steps * nb
    owners_all = (src_brick // nb).reshape(steps, n_s, nb)
    owners_all = jnp.transpose(owners_all, (1, 0, 2)).reshape(n_s, request_total)
    local_rows = (src_brick % nb).reshape(steps, n_s, nb)
    local_rows = jnp.transpose(local_rows, (1, 0, 2)).reshape(n_s, request_total)
    source_rows = (jnp.arange(request_total, dtype=jnp.int32) // nb * nb)[None, :] + local_rows
    earlier = jnp.arange(request_total)[:, None] > jnp.arange(request_total)[None, :]
    same = (owners_all[:, :, None] == owners_all[:, None, :]) & earlier[None]
    rank = jnp.sum(same.astype(jnp.int32), axis=2)
    matched = (owners_all == self_index)[:, :, None] & (
        rank[:, :, None] == jnp.arange(cap)[None, None, :]
    )
    row_index = jnp.sum(matched.astype(jnp.int32) * source_rows[:, :, None], axis=1)
    pick = lax.dynamic_index_in_dim(owners_all * cap + rank, self_index, 0, keepdims=False)
    return row_index.reshape(n_s * cap), pick


def local(
    tokens, src_brick, merge_num, gain_attn, w_query, w_key, w_value, w_out, gain_mlp, w_in, w_back
):
    nb, bt, d = tokens.shape[1:]
    ff = w_in.shape[1]
    n_s, n_f = lax.axis_size("space"), lax.axis_size("frame")
    self_index = lax.axis_index("space")
    cap = max(2, (n_f - 1) * nb // n_s + 1)
    span = bt // n_f
    cr = min(CHUNK, span)
    nc = span // cr
    mine = lax.dynamic_slice_in_dim(merge_num, self_index * nb, nb, 1)
    weights = (mine.astype(F32) * 0.25).reshape(-1)
    row_index, pick = slot_tables(src_brick, n_s, nb, cap, self_index)
    m = n_f * nb * cr
    smem = pl.BlockSpec(memory_space=pltpu.SMEM)
    vmem = pl.BlockSpec(memory_space=pltpu.VMEM)
    hbm = pl.BlockSpec(memory_space=pl.ANY)
    dma = pltpu.SemaphoreType.DMA
    scratch = (
        [pltpu.VMEM((n_f * nb, cr, d), BF) for _ in range(nc)]
        + [pltpu.VMEM((n_s * cap, cr, d), BF) for _ in range(2 * nc)]
        + [pltpu.VMEM((n_f, nb, cr, d), BF) for _ in range(nc)]
        + [pltpu.VMEM((d, d), BF)] * 4
        + [pltpu.VMEM((d, ff), BF), pltpu.VMEM((ff, d), BF)]
        + [pltpu.VMEM((m, d), BF)] * 5
        + [pltpu.VMEM((m, d), F32)]
        + [dma((nc, n_f)), dma((nc, n_f)), dma((nc, n_s)), dma((nc, n_s))]
        + [dma((nc, n_f)), dma((nc, n_f)), dma((nc,)), dma((nc,)), dma((6,))]
    )
    dims = (n_f, n_s, nb, cr, nc, cap, d)
    return pl.pallas_call(
        functools.partial(kernel, dims),
        out_shape=jax.ShapeDtypeStruct(tokens.shape, tokens.dtype),
        in_specs=[smem] * 3 + [hbm] + [vmem] * 2 + [hbm] * 6,
        out_specs=hbm,
        scratch_shapes=scratch,
        compiler_params=pltpu.CompilerParams(
            collective_id=0, has_side_effects=True, vmem_limit_bytes=56 << 20
        ),
        name="temporal_block",
    )(
        row_index, pick, weights, tokens, gain_attn.reshape(1, d), gain_mlp.reshape(1, d),
        w_query, w_key, w_value, w_out, w_in, w_back,
    )


def solution(mesh):
    tok_spec = P("frame", ("groups", "space"), None, None)
    in_specs = (tok_spec, P(None, "groups"), P(None, "groups")) + (P(),) * 8
    return jax.shard_map(
        local, mesh=mesh, in_specs=in_specs, out_specs=tok_spec, check_vma=False
    )
```
